32 devices in a mesh: grp: 2 (over y), gx: 4 (over z), gy: 2 (over x), gz: 2 (over core).
Axes of the slice: x: 2, y: 2, z: 4, core: 2. Of those that a mesh axis runs over, the one named last changes fastest.
Arguments:
- design: int32 [16, 16, 256], P(('grp', 'gx'), 'gy', 'gz'), parts along dimension 0, may hold values from 0 to 15
- supports: int32 [16, 16, 256], P(('grp', 'gx'), 'gy', 'gz'), parts along dimension 0, may hold values 0 or 1
- body_load: float32 [12, 3, 8, 16, 256], P('grp', None, 'gx', 'gy', 'gz'), parts along dimension 0, may hold values from -6 to 6
- start: float32 [12, 3, 8, 16, 256], P('grp', None, 'gx', 'gy', 'gz'), parts along dimension 0, may hold values from -1.8 to 1.8
- load_nodes: int32 [12, 16], P('grp'), parts along dimension 0, may hold values from 0 to 32767
- load_values: float32 [12, 16, 3], P('grp'), parts along dimension 0, may hold values from -24 to 24
Outputs:
- solution: float32 [12, 3, 8, 16, 256], P('grp', None, 'gx', 'gy', 'gz'), parts along dimension 0
- residual: float32 [12, 3, 8, 16, 256], P('grp', None, 'gx', 'gy', 'gz'), parts along dimension 0
The draws below stay inside these ranges and needn't reach their ends.
There are 2 independent parts, one for each index of `grp`. The reference program is written for one: setup_inputs(seed, part) draws one part's arguments, and reference() takes and returns one part's arrays. A program takes and returns all parts, laid end to end along the dimension named above; each array names one. Nothing has to cross between parts.
Inputs may be any that keep to these rules, and one draw needn't show every extreme that they name: `supports`: 1 where all three displacements of the node are held fixed. `load_nodes`: flat index (i * 16 + j) * 256 + k of a loaded node; a node may be named several times.
All inputs are finite; a program needn't handle non-finite values. No bound on the sum of `supports` on one device may be relied on, other than what follows from the above.
Results may differ from the reference program's by a relative error of at most 0.0003.
Values sent between devices are 32-bit elements; how exact they have to be, the bound alone decides.
A program may use at most 64 MiB of HBM per device.

```python
import jax
import jax.numpy as jnp
import numpy as np
from jax import lax

CASES = 6
LOADS = 16
LEVELS = 16
ITERS = 2
NX = 8
NY = 16
NZ = 256


def plant(values, key, low, largest):
    place = [jax.random.randint(jax.random.fold_in(key, axis), (), 0, length) for axis, length in enumerate(values.shape)]
    main_axis = values.shape.index(max(values.shape))
    neighbour = place[:main_axis] + [(place[main_axis] + 1) % values.shape[main_axis]] + place[main_axis + 1:]
    return values.at[tuple(place)].set(low).at[tuple(neighbour)].set(largest)


def block_scale(own_key, shape, shards, smallest, top_value):
    gain = 1.0
    for dim, parts in shards:
        heights = jax.random.uniform(jax.random.fold_in(jax.random.fold_in(own_key, 6), dim), (parts,), jnp.float32, smallest / len(shards), top_value / len(shards))
        gain = gain * jnp.repeat(jnp.exp(heights), shape[dim] // parts).reshape((-1,) + (1,) * (len(shape) - 1 - dim))
    return gain


def centred(rng, shape, scale, reach, pieces=(), kind=jnp.bfloat16):
    result = jax.random.normal(rng, shape, jnp.float32) * scale
    if len(pieces) > 0:
        result = block_scale(rng, shape, pieces, -0.22, 0.18) * result
    return jnp.clip(result, min=-reach, max=reach).astype(kind)


def setup_inputs(seed: int = 0, part: int = 0) -> dict:
    key_of = jax.random.split(jax.random.key(seed), 7)
    part_keys = jax.random.split(jax.random.fold_in(key_of[6], part), 7)
    return {
        "design": plant(jax.random.randint(part_keys[0], (NX, NY, NZ), 0, LEVELS), jax.random.fold_in(part_keys[0], 1), 0, LEVELS - 1).astype(jnp.int32),
        "supports": plant((jax.random.randint(part_keys[1], (NX, NY, NZ), 0, 16) < 1).astype(jnp.int32), jax.random.fold_in(part_keys[1], 1), 0, 1),
        "body_load": centred(part_keys[2], (CASES, 3, NX, NY, NZ), 1.0, 6.0, ((2, 4), (3, 2), (4, 2)), jnp.float32),
        "start": centred(part_keys[3], (CASES, 3, NX, NY, NZ), 0.3, 1.8, ((2, 4), (3, 2), (4, 2)), jnp.float32),
        "load_nodes": plant(jax.random.randint(part_keys[4], (CASES, LOADS), 0, NX * NY * NZ), jax.random.fold_in(part_keys[4], 1), 0, (NX * NY * NZ) - 1).astype(jnp.int32),
        "load_values": centred(part_keys[5], (CASES, LOADS, 3), 4.0, 24.0, (), jnp.float32),
    }


soft_modulus = 0.05
poisson_ratio = 0.3
highest = lax.Precision.HIGHEST

def corner_list():
    return [(first, second, third) for first in (0, 1) for second in (0, 1) for third in (0, 1)]

def element_matrix():
    ratio = poisson_ratio
    lame_first = ratio / ((1.0 + ratio) * (1.0 - 2.0 * ratio))
    shear_modulus = 1.0 / (2.0 * (1.0 + ratio))
    elastic = np.zeros((6, 6))
    elastic[:3, :3] = lame_first
    for axis_dim in range(3):
        elastic[axis_dim, axis_dim] += 2.0 * shear_modulus
        elastic[3 + axis_dim, 3 + axis_dim] = shear_modulus
    gauss_points = [0.5 - 0.5 / np.sqrt(3.0), 0.5 + 0.5 / np.sqrt(3.0)]
    corners = corner_list()
    matrix_total = np.zeros((24, 24))
    for first_point in gauss_points:
        for second_point in gauss_points:
            for third_point in gauss_points:
                points = (first_point, second_point, third_point)
                strain = np.zeros((6, 24))
                for number, corner in enumerate(corners):
                    values = [points[axis_dim] if corner[axis_dim] else 1.0 - points[axis_dim] for axis_dim in range(3)]
                    slopes = [1.0 if corner[axis_dim] else -1.0 for axis_dim in range(3)]
                    grad_first = slopes[0] * values[1] * values[2]
                    grad_second = values[0] * slopes[1] * values[2]
                    grad_third = values[0] * values[1] * slopes[2]
                    column = 3 * number
                    strain[0, column] = grad_first
                    strain[1, column + 1] = grad_second
                    strain[2, column + 2] = grad_third
                    strain[3, column] = grad_second
                    strain[3, column + 1] = grad_first
                    strain[4, column + 1] = grad_third
                    strain[4, column + 2] = grad_second
                    strain[5, column] = grad_third
                    strain[5, column + 2] = grad_first
                matrix_total = matrix_total + strain.T @ elastic @ strain / 8.0
    return jnp.asarray(matrix_total, dtype=jnp.float32)

def stiffness_of(design):
    density = (design.astype(jnp.float32) + 1.0) / LEVELS
    return soft_modulus + (1.0 - soft_modulus) * density * density * density

def crop(array, width):
    return array[..., width:array.shape[-3] - width, width:array.shape[-2] - width, width:array.shape[-1] - width]

def pad_grid(array):
    widths = [(0, 0)] * (array.ndim - 3) + [(1, 1)] * 3
    return jnp.pad(array, widths)

def stiff_apply(padded, moduli, element_stiffness):
    span_first, span_second, span_third = padded.shape[-3:]
    corners = corner_list()
    results = []
    for member in range(padded.shape[0]):
        single = padded[member]
        stacked = jnp.concatenate([single[:, corner[0]:span_first - 1 + corner[0], corner[1]:span_second - 1 + corner[1], corner[2]:span_third - 1 + corner[2]] for corner in corners], axis=0)
        forces = jnp.einsum('ij,jxyz->ixyz', element_stiffness, stacked, precision=highest)
        forces = forces * moduli[None, :span_first - 1, :span_second - 1, :span_third - 1]
        accumulated = jnp.zeros((3, span_first - 2, span_second - 2, span_third - 2), jnp.float32)
        for number, corner in enumerate(corners):
            accumulated = accumulated + forces[3 * number:3 * number + 3, 1 - corner[0]:span_first - 1 - corner[0], 1 - corner[1]:span_second - 1 - corner[1], 1 - corner[2]:span_third - 1 - corner[2]]
        results.append(accumulated)
    return jnp.stack(results)

def operate(padded, moduli, movable_pad, element_stiffness):
    forces = stiff_apply(padded * movable_pad, moduli, element_stiffness)
    inner = crop(movable_pad, 1)
    return inner * forces + (1.0 - inner) * crop(padded, 1)

def inverse_diagonal(moduli, movable_inner, element_stiffness):
    span_first, span_second, span_third = moduli.shape
    adjacent = jnp.zeros((span_first - 2, span_second - 2, span_third - 2), jnp.float32)
    for corner in corner_list():
        adjacent = adjacent + moduli[1 - corner[0]:span_first - 1 - corner[0], 1 - corner[1]:span_second - 1 - corner[1], 1 - corner[2]:span_third - 1 - corner[2]]
    guarded = jnp.where(movable_inner > 0, adjacent, 1.0)
    return movable_inner / (element_stiffness[0, 0] * guarded) + (1.0 - movable_inner)

def gram_matrix(first, second):
    return jnp.einsum('iaxyz,jaxyz->ij', first, second, precision=highest)

def combine(fields, coeffs):
    return jnp.einsum('jaxyz,ji->iaxyz', fields, coeffs, precision=highest)

def small_solve(matrix, right):
    factor = jnp.linalg.cholesky(matrix)
    middle = lax.linalg.triangular_solve(factor, right, left_side=True, lower=True)
    return lax.linalg.triangular_solve(factor, middle, left_side=True, lower=True, transpose_a=True)

def add_points(plane, nodes, values):
    return plane.at[:, nodes].add(values.T)

def reference(design, supports, body_load, start, load_nodes, load_values):
    element_stiffness = element_matrix()
    stiffness = stiffness_of(design)
    movable = 1.0 - supports.astype(jnp.float32)
    moduli = pad_grid(stiffness)
    movable_pad = pad_grid(movable)
    flat = body_load.reshape(body_load.shape[0], 3, -1)
    loaded = jax.vmap(add_points)(flat, load_nodes, load_values).reshape(body_load.shape)
    loading = movable * loaded
    residual = loading - operate(pad_grid(start), moduli, movable_pad, element_stiffness)
    scaling = inverse_diagonal(moduli, movable, element_stiffness)
    direction = scaling * residual
    solution = start
    for turn_index in range(ITERS):
        applied = operate(pad_grid(direction), moduli, movable_pad, element_stiffness)
        curvature = gram_matrix(direction, applied)
        projection = gram_matrix(direction, residual)
        step_size = small_solve(curvature, projection)
        solution = solution + combine(direction, step_size)
        updated = residual - combine(applied, step_size)
        if turn_index + 1 < ITERS:
            scaled = scaling * updated
            coupling = gram_matrix(applied, scaled)
            direction = scaled + combine(direction, -small_solve(curvature, coupling))
        residual = updated
    return (solution, residual)
```

```python
import functools
import itertools

import jax
import jax.numpy as jnp
import numpy as np
from jax import lax
from jax.experimental import pallas as pl
from jax.experimental.pallas import tpu as pltpu
from jax.sharding import PartitionSpec as P

LEVELS = 16
AXES = ("gx", "gy", "gz")
MESH = pl.DeviceIdType.MESH
soft_modulus = 0.05
poisson_ratio = 0.3
DIRECTIONS = [d for d in itertools.product((-1, 0, 1), repeat=3) if d != (0, 0, 0)]


def corner_list():
    return [(first, second, third) for first in (0, 1) for second in (0, 1) for third in (0, 1)]


def element_matrix():
    lame_first = poisson_ratio / ((1.0 + poisson_ratio) * (1.0 - 2.0 * poisson_ratio))
    shear_modulus = 1.0 / (2.0 * (1.0 + poisson_ratio))
    elastic = np.zeros((6, 6))
    elastic[:3, :3] = lame_first
    for axis_dim in range(3):
        elastic[axis_dim, axis_dim] += 2.0 * shear_modulus
        elastic[3 + axis_dim, 3 + axis_dim] = shear_modulus
    gauss_points = [0.5 - 0.5 / np.sqrt(3.0), 0.5 + 0.5 / np.sqrt(3.0)]
    corners = corner_list()
    matrix_total = np.zeros((24, 24))
    for first_point in gauss_points:
        for second_point in gauss_points:
            for third_point in gauss_points:
                points = (first_point, second_point, third_point)
                strain = np.zeros((6, 24))
                for number, corner in enumerate(corners):
                    values = [
                        points[axis_dim] if corner[axis_dim] else 1.0 - points[axis_dim]
                        for axis_dim in range(3)
                    ]
                    slopes = [1.0 if corner[axis_dim] else -1.0 for axis_dim in range(3)]
                    grad_first = slopes[0] * values[1] * values[2]
                    grad_second = values[0] * slopes[1] * values[2]
                    grad_third = values[0] * values[1] * slopes[2]
                    column = 3 * number
                    strain[0, column] = grad_first
                    strain[1, column + 1] = grad_second
                    strain[2, column + 2] = grad_third
                    strain[3, column] = grad_second
                    strain[3, column + 1] = grad_first
                    strain[4, column + 1] = grad_third
                    strain[4, column + 2] = grad_second
                    strain[5, column] = grad_third
                    strain[5, column + 2] = grad_first
                matrix_total = matrix_total + strain.T @ elastic @ strain / 8.0
    return matrix_total


def mode_matrix():
    matrix = element_matrix()
    pair = np.array([[1.0, 1.0], [-1.0, 1.0]])
    basis = np.kron(np.kron(np.kron(pair, pair), pair), np.eye(3))
    inverse = np.linalg.inv(basis)
    modes = inverse.T @ matrix @ inverse
    modes[np.abs(modes) < 1e-9] = 0.0
    return float(np.float32(matrix[0, 0])), modes


def triangle(count):
    return [(i, j) for i in range(count) for j in range(i, count)]


def spd_factor(entry, count):
    lower, inverse = {}, []
    work = {(i, j): entry(j, i) for i in range(count) for j in range(i + 1)}
    for k in range(count):
        inverse.append(1.0 / work[k, k])
        for i in range(k + 1, count):
            lower[i, k] = work[i, k] * inverse[k]
        for i in range(k + 1, count):
            for j in range(k + 1, i + 1):
                work[i, j] = work[i, j] - lower[i, k] * work[j, k]
    return lower, inverse


def spd_solve(factor, right, count):
    lower, inverse = factor
    result = {}
    for column in range(count):
        values = [right[row, column] for row in range(count)]
        for i in range(count):
            for k in range(i):
                values[i] = values[i] - lower[i, k] * values[k]
        values = [value * scale for value, scale in zip(values, inverse)]
        for i in reversed(range(count)):
            for k in range(i + 1, count):
                values[i] = values[i] - lower[k, i] * values[k]
        for row in range(count):
            result[row, column] = values[row]
    return result


def kernel(
    sizes, stages,
    design, supports, body, start, nodes, values,
    solution_ref, residual_ref,
    field, rowtx, rowrx, coltx, colrx, movable_ref, scale_ref, modulus,
    resid, direct, image, second, second_image, grams, coef, sumtx, sumrx,
    halo_send, halo_recv, sum_send, sum_recv,
):
    cases, _, n0, n1, n2 = start.shape
    loads = nodes.shape[1]
    fields = 3 * cases
    rows, lanes = field.shape[-2:]
    corner_stiffness, modes = mode_matrix()
    place = {axis: lax.axis_index(axis) for axis in AXES}

    def present(d):
        inside = None
        for axis, step in zip(AXES, d):
            if step:
                test = (place[axis] > 0) if step < 0 else (place[axis] < sizes[axis] - 1)
                inside = test if inside is None else jnp.logical_and(inside, test)
        return inside

    def target(d):
        return {axis: place[axis] + step for axis, step in zip(AXES, d) if step}

    def possible(d):
        return all(step == 0 or sizes[axis] > 1 for axis, step in zip(AXES, d))

    directions = [d for d in DIRECTIONS if possible(d)]

    def members(stage):
        index, size = 0, 1
        for axis in stage:
            index = index * sizes[axis] + place[axis]
            size = size * sizes[axis]
        return index, size

    def peer(stage, number):
        out = {}
        for axis in reversed(stage):
            out[axis] = lax.rem(number, sizes[axis])
            number = lax.div(number, sizes[axis])
        return out

    barrier = pltpu.get_barrier_semaphore()
    if any(sizes[axis] > 1 for axis in AXES):
        rowrx[...] = jnp.zeros_like(rowrx)
        colrx[...] = jnp.zeros_like(colrx)
        for turn in range(3):
            zero = jnp.zeros((field.shape[1], 1, n1, n2), jnp.float32)
            field[turn, :, 0:1, 0:n1, 0:n2] = zero
            field[turn, :, n0 + 1 : n0 + 2, 0:n1, 0:n2] = zero
    expected = 0
    for stage in stages:
        index, size = members(stage)
        expected = expected + (size - 1)
        for offset in range(1, size):
            pl.semaphore_signal(
                barrier, inc=1, device_id=peer(stage, lax.rem(index + offset, size)), device_id_type=MESH
            )
    if len(stages) > 1:
        for d in directions:
            expected = expected + present(d).astype(jnp.int32)

            @pl.when(present(d))
            def _():
                pl.semaphore_signal(barrier, inc=1, device_id=target(d), device_id_type=MESH)

    lane = lax.broadcasted_iota(jnp.int32, (n1, 128), 1)
    row = lax.broadcasted_iota(jnp.int32, (8, n2), 0)

    def planes(step):
        if step == 0:
            return pl.ds(0, n0), pl.ds(1, n0)
        if step > 0:
            return pl.ds(n0 - 1, 1), pl.ds(0, 1)
        return pl.ds(0, 1), pl.ds(n0 + 1, 1)

    def opposite(d):
        return tuple(-step for step in d)

    def halo_copy(turn, number, count, toward=None):
        d = directions[number]
        source, goal = planes(d[0])
        if d[2]:
            side = 0 if d[2] > 0 else 1
            src = coltx.at[turn, side, source]
            dst = colrx.at[turn, side, 1 - d[1], goal]
        elif d[1]:
            side = 0 if d[1] > 0 else 1
            src = rowtx.at[turn, side, source]
            dst = rowrx.at[turn, side, goal]
        else:
            inner = pl.ds(n0 if d[0] > 0 else 1, 1)
            part = (turn, pl.ds(0, count))
            src = field.at[part + (inner, pl.ds(0, n1), pl.ds(0, n2))]
            dst = field.at[part + (goal, pl.ds(0, n1), pl.ds(0, n2))]
        return pltpu.make_async_remote_copy(
            src_ref=src, dst_ref=dst,
            send_sem=halo_send.at[turn, number], recv_sem=halo_recv.at[turn, number],
            device_id=target(toward or d), device_id_type=MESH,
        )

    def pack(turn, count):
        for p in range(n0):
            low = jnp.zeros((n1, 128), jnp.float32)
            high = jnp.zeros((n1, 128), jnp.float32)
            for f in range(count):
                block = field[turn, f, 1 + p, 0:n1, 0:n2]
                rowtx[turn, 0, p, f : f + 1, :] = block[n1 - 1 : n1]
                rowtx[turn, 1, p, f : f + 1, :] = block[0:1]
                high = jnp.where(lane == f, block[:, n2 - 1 : n2], high)
                low = jnp.where(lane == f, block[:, 0:1], low)
            coltx[turn, 0, p] = high
            coltx[turn, 1, p] = low

    def halo_start(turn, count):
        for number, d in enumerate(directions):
            @pl.when(present(d))
            def _():
                halo_copy(turn, number, count).start()

    def halo_finish(turn, count):
        for number, d in enumerate(directions):
            @pl.when(present(opposite(d)))
            def _():
                halo_copy(turn, number, count, opposite(d)).wait_recv()

        def unpack(q, carry):
            for f in range(count):
                low, high = rowrx[turn, 0, q, f : f + 1, :], rowrx[turn, 1, q, f : f + 1, :]
                field[turn, f, q, n1 : n1 + 8, 0:n2] = jnp.where(row == 0, high, jnp.where(row == 7, low, 0.0))
                for yy, top, size in ((1, 0, n1), (None, n1, 8)):
                    if yy is None:
                        first = colrx[turn, 1, 2, q, 0:1, f : f + 1]
                        last = colrx[turn, 1, 0, q, n1 - 1 : n1, f : f + 1]
                        after = jnp.where(row[:, 0:1] == 0, first, jnp.where(row[:, 0:1] == 7, last, 0.0))
                        first = colrx[turn, 0, 2, q, 0:1, f : f + 1]
                        last = colrx[turn, 0, 0, q, n1 - 1 : n1, f : f + 1]
                        before = jnp.where(row[:, 0:1] == 0, first, jnp.where(row[:, 0:1] == 7, last, 0.0))
                    else:
                        after = colrx[turn, 1, 1, q, :, f : f + 1]
                        before = colrx[turn, 0, 1, q, :, f : f + 1]
                    where = lane[0:1] if size != n1 else lane
                    field[turn, f, q, top : top + size, n2 : n2 + 128] = jnp.where(
                        where == 0, after, jnp.where(where == 127, before, 0.0)
                    )
            return carry

        lax.fori_loop(0, n0 + 2, unpack, 0)

    def sum_start(turn, step, tile):
        stage = stages[step]
        index, size = members(stage)
        sumtx[turn, step] = tile
        sumrx[turn, step, pl.ds(index, 1)] = tile[None]
        for offset in range(1, size):
            sum_copy(turn, step, offset).start()

    def sum_copy(turn, step, offset):
        stage = stages[step]
        index, size = members(stage)
        return pltpu.make_async_remote_copy(
            src_ref=sumtx.at[turn, step],
            dst_ref=sumrx.at[turn, step, index],
            send_sem=sum_send.at[turn, step, offset], recv_sem=sum_recv.at[turn, step, offset],
            device_id=peer(stage, lax.rem(index + offset, size)), device_id_type=MESH,
        )

    def sum_finish(turn):
        for step, stage in enumerate(stages):
            _, size = members(stage)
            for offset in range(1, size):
                sum_copy(turn, step, offset).wait_recv()
            total = sumrx[turn, step, 0]
            for number in range(1, size):
                total = total + sumrx[turn, step, number]
            if step + 1 < len(stages):
                sum_start(turn, step + 1, total)
        spots = lax.broadcasted_iota(jnp.int32, (grams.shape[0], 128), 0)
        across = lax.broadcasted_iota(jnp.int32, (grams.shape[0], 128), 1)
        spread = jnp.where(spots == across, total[0:1], 0.0)
        grams[...] = jnp.broadcast_to(jnp.sum(spread, axis=1, keepdims=True), grams.shape)

    def gram_rows(first, other, pairs, base):
        for number, (i, j) in enumerate(pairs):
            product = None
            for d in range(3):
                for p in range(n0):
                    term = first[i, d, p] * other[j, d, p]
                    product = term if product is None else product + term
            grams[base + number : base + number + 1, :] = jnp.sum(product, axis=0, keepdims=True)

    def gram_tile():
        return lax.dot_general(
            jnp.ones((8, 128), jnp.float32), grams[...], (((1,), (1,)), ((), ())),
            precision=lax.Precision.HIGHEST, preferred_element_type=jnp.float32,
        )

    def apply(turn, finish):
        def one(c, carry):
            def plane(q):
                parts = {}
                for d in range(3):
                    v = field[turn, 3 * c + d, q]
                    after = pltpu.roll(v, lanes - 1, 1)
                    for cc, along in enumerate((v + after, after - v)):
                        beyond = pltpu.roll(along, rows - 1, 0)
                        parts[d, 0, cc] = along + beyond
                        parts[d, 1, cc] = beyond - along
                return parts

            before, behind = plane(0), None
            for q in range(n0 + 1):
                ahead = plane(q + 1)
                strain = {}
                for d, b, cc in ahead:
                    strain[4 * 0 + 2 * b + cc, d] = ahead[d, b, cc] + before[d, b, cc]
                    strain[4 * 1 + 2 * b + cc, d] = ahead[d, b, cc] - before[d, b, cc]
                stiff = modulus[q]
                stress = {}
                for number in range(8):
                    for d in range(3):
                        total = None
                        for other in range(8):
                            for e in range(3):
                                weight = modes[3 * number + d, 3 * other + e]
                                if weight != 0.0:
                                    term = float(weight) * strain[other, e]
                                    total = term if total is None else total + term
                        stress[number, d] = None if total is None else total * stiff

                def side(sign):
                    out = {}
                    for d in range(3):
                        for b in range(2):
                            for cc in range(2):
                                total, change = stress[2 * b + cc, d], stress[4 + 2 * b + cc, d]
                                if total is None:
                                    out[d, b, cc] = change if sign > 0 else -change
                                else:
                                    out[d, b, cc] = total + change if sign > 0 else total - change
                    return out

                if q > 0:
                    near = side(-1)
                    for d in range(3):
                        folded = []
                        for cc in range(2):
                            flat = behind[d, 0, cc] + near[d, 0, cc]
                            tilt = behind[d, 1, cc] + near[d, 1, cc]
                            folded.append((flat - tilt)[0:n1] + pltpu.roll(flat + tilt, 1, 0)[0:n1])
                        force = (folded[0] - folded[1])[:, 0:n2]
                        force = force + pltpu.roll(folded[0] + folded[1], 1, 1)[:, 0:n2]
                        finish(c, d, q - 1, force)
                if q < n0:
                    behind = side(1)
                before = ahead
            return carry

        lax.fori_loop(0, cases, one, 0)

    for p in range(n0):
        density = (design[p].astype(jnp.float32) + 1.0) * (1.0 / LEVELS)
        movable_ref[p] = 1.0 - supports[p].astype(jnp.float32)
        field[0, fields, 1 + p, 0:n1, 0:n2] = soft_modulus + (1.0 - soft_modulus) * density * density * density
    for c in range(cases):
        for d in range(3):
            for p in range(n0):
                field[0, 3 * c + d, 1 + p, 0:n1, 0:n2] = movable_ref[p] * start[c, d, p]
    pack(0, fields + 1)
    pl.semaphore_wait(barrier, expected)
    halo_start(0, fields + 1)

    along1, along2 = n1 * sizes["gy"], n2 * sizes["gz"]

    def load_case(c, carry):
        for p in range(n0):
            first = place["gx"] * n0 + p
            second_index = place["gy"] * n1 + lax.broadcasted_iota(jnp.int32, (n1, n2), 0)
            third = place["gz"] * n2 + lax.broadcasted_iota(jnp.int32, (n1, n2), 1)
            number = (first * along1 + second_index) * along2 + third
            sums = [body[c, d, p] for d in range(3)]
            for l in range(loads):
                hit = number == nodes[c, l]
                for d in range(3):
                    sums[d] = sums[d] + jnp.where(hit, values[c, l * 3 + d], 0.0)
            for d in range(3):
                resid[c, d, p] = movable_ref[p] * sums[d]
        return carry

    lax.fori_loop(0, cases, load_case, 0)
    halo_finish(0, fields + 1)
    for q in range(n0 + 1):
        modulus[q] = field[0, fields, q]
    for p in range(n0):
        total = modulus[p] + modulus[p + 1]
        total = total + pltpu.roll(total, 1, 0)
        total = total + pltpu.roll(total, 1, 1)
        movable = movable_ref[p]
        guarded = jnp.where(movable > 0, total[0:n1, 0:n2], 1.0)
        scale_ref[p] = movable / (corner_stiffness * guarded) + (1.0 - movable)

    def first_finish(c, d, p, force):
        movable = movable_ref[p]
        value = resid[c, d, p] - (movable * force + (1.0 - movable) * start[c, d, p])
        resid[c, d, p] = value
        direction = scale_ref[p] * value
        direct[c, d, p] = direction
        field[1, 3 * c + d, 1 + p, 0:n1, 0:n2] = movable * direction

    apply(0, first_finish)
    pack(1, fields)
    halo_start(1, fields)
    pairs = triangle(cases)
    count = len(pairs)
    grams[...] = jnp.zeros_like(grams)
    gram_rows(direct, resid, pairs, count)
    halo_finish(1, fields)

    def second_finish(c, d, p, force):
        movable = movable_ref[p]
        value = movable * force + (1.0 - movable) * direct[c, d, p]
        image[c, d, p] = value
        scaled = scale_ref[p] * value
        second[c, d, p] = scaled
        field[2, 3 * c + d, 1 + p, 0:n1, 0:n2] = movable * scaled

    apply(1, second_finish)
    pack(2, fields)
    halo_start(2, fields)
    gram_rows(direct, image, pairs, 0)
    gram_rows(image, second, pairs, 2 * count)
    sum_start(0, 0, gram_tile())
    halo_finish(2, fields)

    def third_finish(c, d, p, force):
        movable = movable_ref[p]
        second_image[c, d, p] = movable * force + (1.0 - movable) * second[c, d, p]

    apply(2, third_finish)
    sum_finish(0)

    def entries(base):
        spot = {}
        for number, (i, j) in enumerate(pairs):
            spot[i, j] = spot[j, i] = base + number
        return lambda i, j: grams[spot[i, j] : spot[i, j] + 1, :]

    everyone = [(i, j) for i in range(cases) for j in range(cases)]
    curvature, projection, crossing = entries(0), entries(count), entries(2 * count)
    factor = spd_factor(curvature, cases)
    step = spd_solve(factor, {pair: projection(*pair) for pair in everyone}, cases)
    coupling = {}
    for i, j in everyone:
        total = curvature(j, i)
        for k in range(cases):
            total = total - crossing(i, k) * step[k, j]
        coupling[i, j] = total
    beta = spd_solve(factor, coupling, cases)
    for number, pair in enumerate(everyone):
        coef[0, number] = jnp.broadcast_to(step[pair], coef.shape[2:])
        coef[1, number] = jnp.broadcast_to(beta[pair], coef.shape[2:])

    def first_update(number, carry):
        d, p = lax.div(number, n0), lax.rem(number, n0)
        scale = scale_ref[p]
        for i in range(cases):
            gain, loss, kept, moved = start[i, d, p], resid[i, d, p], None, image[i, d, p]
            for j in range(cases):
                alpha, weight = coef[0, j * cases + i], coef[1, j * cases + i]
                gain = gain + direct[j, d, p] * alpha
                loss = loss - image[j, d, p] * alpha
                term = direct[j, d, p] * weight
                kept = term if kept is None else kept + term
                moved = moved - (second_image[j, d, p] * alpha + image[j, d, p] * weight)
            solution_ref[i, d, p] = gain
            residual_ref[i, d, p] = loss
            field[0, 3 * i + d, 1 + p, 0:n1, 0:n2] = scale * loss - kept
            field[1, 3 * i + d, 1 + p, 0:n1, 0:n2] = moved
        for i in range(cases):
            second[i, d, p] = field[0, 3 * i + d, 1 + p, 0:n1, 0:n2]
            second_image[i, d, p] = field[1, 3 * i + d, 1 + p, 0:n1, 0:n2]
        return carry

    halo_drain(halo_copy, directions, present, (0, 1, 2), fields)
    lax.fori_loop(0, 3 * n0, first_update, 0)
    grams[...] = jnp.zeros_like(grams)
    gram_rows(second, second_image, pairs, 0)
    gram_rows(second, residual_ref, everyone, count)
    sum_start(1, 0, gram_tile())
    sum_finish(1)
    curvature = entries(0)
    factor = spd_factor(curvature, cases)
    right = {pair: grams[count + n : count + n + 1, :] for n, pair in enumerate(everyone)}
    step = spd_solve(factor, right, cases)
    for number, pair in enumerate(everyone):
        coef[0, number] = jnp.broadcast_to(step[pair], coef.shape[2:])

    def second_update(number, carry):
        d, p = lax.div(number, n0), lax.rem(number, n0)
        for i in range(cases):
            gain, loss = solution_ref[i, d, p], residual_ref[i, d, p]
            for j in range(cases):
                alpha = coef[0, j * cases + i]
                gain = gain + second[j, d, p] * alpha
                loss = loss - second_image[j, d, p] * alpha
            solution_ref[i, d, p] = gain
            residual_ref[i, d, p] = loss
        return carry

    lax.fori_loop(0, 3 * n0, second_update, 0)
    for turn in range(2):
        for number, stage in enumerate(stages):
            _, size = members(stage)
            for offset in range(1, size):
                sum_copy(turn, number, offset).wait_send()


def halo_drain(halo_copy, directions, present, turns, fields):
    for turn in turns:
        for number, d in enumerate(directions):
            @pl.when(present(d))
            def _():
                halo_copy(turn, number, fields + 1 if turn == 0 else fields).wait_send()


def solution(mesh):
    sizes = {axis: mesh.shape[axis] for axis in AXES}
    group = sizes["gx"] * sizes["gy"] * sizes["gz"]
    stages = [AXES] if group <= 16 else [("gz",), ("gy",), ("gx",)]

    def shards(design, supports, body_load, start, load_nodes, load_values):
        cases, _, n0, n1, n2 = start.shape
        fields = 3 * cases
        padded = -(-(fields + 1) // 8) * 8
        directions = len([d for d in DIRECTIONS if all(s == 0 or sizes[a] > 1 for a, s in zip(AXES, d))])
        widest = max(int(np.prod([sizes[axis] for axis in stage])) for stage in stages)
        f32 = jnp.float32
        vmem, smem = pl.BlockSpec(memory_space=pltpu.VMEM), pl.BlockSpec(memory_space=pltpu.SMEM)
        block = pltpu.VMEM(start.shape, f32)
        gram_count = -(-max(3 * cases * (cases + 1) // 2, cases * (cases + 1) // 2 + cases * cases) // 128) * 128
        scratch = [
            pltpu.VMEM((3, fields + 1, n0 + 2, n1 + 8, n2 + 128), f32),
            pltpu.VMEM((3, 2, n0, padded, n2), f32),
            pltpu.VMEM((3, 2, n0 + 2, padded, n2), f32),
            pltpu.VMEM((3, 2, n0, n1, 128), f32),
            pltpu.VMEM((3, 2, 3, n0 + 2, n1, 128), f32),
            pltpu.VMEM((n0, n1, n2), f32),
            pltpu.VMEM((n0, n1, n2), f32),
            pltpu.VMEM((n0 + 1, n1 + 8, n2 + 128), f32),
            block, block, block, block, block,
            pltpu.VMEM((gram_count, 128), f32),
            pltpu.VMEM((2, cases * cases, n1, n2), f32),
            pltpu.VMEM((2, len(stages), 8, 128), f32),
            pltpu.VMEM((2, len(stages), widest, 8, 128), f32),
            pltpu.SemaphoreType.DMA((3, directions)),
            pltpu.SemaphoreType.DMA((3, directions)),
            pltpu.SemaphoreType.DMA((2, len(stages), widest)),
            pltpu.SemaphoreType.DMA((2, len(stages), widest)),
        ]
        return pl.pallas_call(
            functools.partial(kernel, sizes, stages),
            out_shape=(jax.ShapeDtypeStruct(start.shape, f32), jax.ShapeDtypeStruct(start.shape, f32)),
            in_specs=[vmem] * 4 + [smem] * 2,
            out_specs=(vmem, vmem),
            scratch_shapes=scratch,
            compiler_params=pltpu.CompilerParams(collective_id=0, has_side_effects=True),
        )(design, supports, body_load, start, load_nodes, load_values.reshape(cases, -1))

    in_specs = (
        P(("grp", "gx"), "gy", "gz"),
        P(("grp", "gx"), "gy", "gz"),
        P("grp", None, "gx", "gy", "gz"),
        P("grp", None, "gx", "gy", "gz"),
        P("grp", None),
        P("grp", None, None),
    )
    out_specs = (P("grp", None, "gx", "gy", "gz"), P("grp", None, "gx", "gy", "gz"))
    return jax.shard_map(shards, mesh=mesh, in_specs=in_specs, out_specs=out_specs, check_vma=False)
```

```python
import functools
import itertools

import jax
import jax.numpy as jnp
import numpy as np
from jax import lax
from jax.experimental import pallas as pl
from jax.experimental.pallas import tpu as pltpu
from jax.sharding import PartitionSpec as P

LEVELS = 16
AXES = ("gx", "gy", "gz")
MESH = pl.DeviceIdType.MESH
soft_modulus = 0.05
poisson_ratio = 0.3
SWAP = 2


def neighbours(sizes):
    options = [(0,) if sizes[axis] == 1 else (0, SWAP) if sizes[axis] == 2 else (-1, 0, 1) for axis in AXES]
    return [d for d in itertools.product(*options) if any(d)]


def corner_list():
    return [(first, second, third) for first in (0, 1) for second in (0, 1) for third in (0, 1)]


def element_matrix():
    lame_first = poisson_ratio / ((1.0 + poisson_ratio) * (1.0 - 2.0 * poisson_ratio))
    shear_modulus = 1.0 / (2.0 * (1.0 + poisson_ratio))
    elastic = np.zeros((6, 6))
    elastic[:3, :3] = lame_first
    for axis_dim in range(3):
        elastic[axis_dim, axis_dim] += 2.0 * shear_modulus
        elastic[3 + axis_dim, 3 + axis_dim] = shear_modulus
    gauss_points = [0.5 - 0.5 / np.sqrt(3.0), 0.5 + 0.5 / np.sqrt(3.0)]
    corners = corner_list()
    matrix_total = np.zeros((24, 24))
    for first_point in gauss_points:
        for second_point in gauss_points:
            for third_point in gauss_points:
                points = (first_point, second_point, third_point)
                strain = np.zeros((6, 24))
                for number, corner in enumerate(corners):
                    values = [
                        points[axis_dim] if corner[axis_dim] else 1.0 - points[axis_dim]
                        for axis_dim in range(3)
                    ]
                    slopes = [1.0 if corner[axis_dim] else -1.0 for axis_dim in range(3)]
                    grad_first = slopes[0] * values[1] * values[2]
                    grad_second = values[0] * slopes[1] * values[2]
                    grad_third = values[0] * values[1] * slopes[2]
                    column = 3 * number
                    strain[0, column] = grad_first
                    strain[1, column + 1] = grad_second
                    strain[2, column + 2] = grad_third
                    strain[3, column] = grad_second
                    strain[3, column + 1] = grad_first
                    strain[4, column + 1] = grad_third
                    strain[4, column + 2] = grad_second
                    strain[5, column] = grad_third
                    strain[5, column + 2] = grad_first
                matrix_total = matrix_total + strain.T @ elastic @ strain / 8.0
    return matrix_total


def mode_matrix():
    matrix = element_matrix()
    pair = np.array([[1.0, 1.0], [-1.0, 1.0]])
    basis = np.kron(np.kron(np.kron(pair, pair), pair), np.eye(3))
    inverse = np.linalg.inv(basis)
    modes = inverse.T @ matrix @ inverse
    modes[np.abs(modes) < 1e-9] = 0.0
    return float(np.float32(matrix[0, 0])), modes


def triangle(count):
    return [(i, j) for i in range(count) for j in range(i, count)]


def spd_factor(entry, count):
    lower, inverse = {}, []
    work = {(i, j): entry(j, i) for i in range(count) for j in range(i + 1)}
    for k in range(count):
        inverse.append(1.0 / work[k, k])
        for i in range(k + 1, count):
            lower[i, k] = work[i, k] * inverse[k]
        for i in range(k + 1, count):
            for j in range(k + 1, i + 1):
                work[i, j] = work[i, j] - lower[i, k] * work[j, k]
    return lower, inverse


def spd_solve(factor, right, count):
    lower, inverse = factor
    result = {}
    for column in range(count):
        values = [right[row, column] for row in range(count)]
        for i in range(count):
            for k in range(i):
                values[i] = values[i] - lower[i, k] * values[k]
        values = [value * scale for value, scale in zip(values, inverse)]
        for i in reversed(range(count)):
            for k in range(i + 1, count):
                values[i] = values[i] - lower[k, i] * values[k]
        for row in range(count):
            result[row, column] = values[row]
    return result


def kernel(
    sizes, stages,
    design_hbm, supports_hbm, body_hbm, start_hbm, nodes, values,
    solution_ref, residual_ref, design, supports, body, start,
    field, rowtx, rowrx, coltx, colrx, movable_ref, scale_ref, modulus,
    resid, direct, image, second, second_image, grams, coef, sumtx, sumrx,
    halo_send, halo_recv, sum_send, sum_recv, load_sem,
):
    cases, _, n0, n1, n2 = start.shape
    loads = nodes.shape[1]
    fields = 3 * cases
    rows, lanes = field.shape[-2:]
    corner_stiffness, modes = mode_matrix()
    place = {axis: lax.axis_index(axis) for axis in AXES}

    def present(d):
        inside = None
        for axis, step in zip(AXES, d):
            if step in (-1, 1):
                test = (place[axis] > 0) if step < 0 else (place[axis] < sizes[axis] - 1)
                inside = test if inside is None else jnp.logical_and(inside, test)
        return inside

    def when(condition, run):
        if condition is None:
            run()
        else:
            pl.when(condition)(run)

    def target(d):
        return {
            axis: 1 - place[axis] if step == SWAP else place[axis] + step
            for axis, step in zip(AXES, d) if step
        }

    def opposite(d):
        return tuple(step if step == SWAP else -step for step in d)

    directions = neighbours(sizes)
    faces = [d for d in directions if d[0] and not d[1] and not d[2]]
    packed = [d for d in directions if d not in faces]

    def members(stage):
        index, size = 0, 1
        for axis in stage:
            index = index * sizes[axis] + place[axis]
            size = size * sizes[axis]
        return index, size

    def peer(stage, number):
        out = {}
        for axis in reversed(stage):
            out[axis] = lax.rem(number, sizes[axis])
            number = lax.div(number, sizes[axis])
        return out

    loaded = [
        pltpu.make_async_copy(source, goal, load_sem.at[number])
        for number, (source, goal) in enumerate(
            ((start_hbm, start), (supports_hbm, supports), (design_hbm, design), (body_hbm, body))
        )
    ]
    for copy in loaded:
        copy.start()
    barrier = pltpu.get_barrier_semaphore()
    if any(sizes[axis] > 1 for axis in AXES):
        rowrx[...] = jnp.zeros_like(rowrx)
        colrx[...] = jnp.zeros_like(colrx)
        for turn in range(3):
            zero = jnp.zeros((field.shape[1], 1, n1, n2), jnp.float32)
            field[turn, :, 0:1, 0:n1, 0:n2] = zero
            field[turn, :, n0 + 1 : n0 + 2, 0:n1, 0:n2] = zero
    expected = 0
    for stage in stages:
        index, size = members(stage)
        expected = expected + (size - 1)
        for offset in range(1, size):
            pl.semaphore_signal(
                barrier, inc=1, device_id=peer(stage, lax.rem(index + offset, size)), device_id_type=MESH
            )
    if len(stages) > 1:
        for d in directions:
            exists = present(d)
            expected = expected + (1 if exists is None else exists.astype(jnp.int32))

            def greet():
                pl.semaphore_signal(barrier, inc=1, device_id=target(d), device_id_type=MESH)

            when(exists, greet)

    lane = lax.broadcasted_iota(jnp.int32, (n1, 128), 1)
    row = lax.broadcasted_iota(jnp.int32, (8, n2), 0)

    def planes(step):
        if step == 0:
            return pl.ds(0, n0), pl.ds(1, n0)
        if step == SWAP:
            return pl.ds((n0 - 1) * (1 - place["gx"]), 1), pl.ds((n0 + 1) * place["gx"], 1)
        if step > 0:
            return pl.ds(n0 - 1, 1), pl.ds(0, 1)
        return pl.ds(0, 1), pl.ds(n0 + 1, 1)

    def side_of(axis, step):
        return place[axis] if step == SWAP else (0 if step > 0 else 1)

    def remote(turn, d, src, dst, toward):
        number = directions.index(d)
        return pltpu.make_async_remote_copy(
            src_ref=src, dst_ref=dst,
            send_sem=halo_send.at[number], recv_sem=halo_recv.at[turn, number],
            device_id=target(toward or d), device_id_type=MESH,
        )

    def pack_copy(turn, d, toward=None):
        source, goal = planes(d[0])
        if d[2]:
            side = side_of("gz", d[2])
            level = 2 * place["gy"] if d[1] == SWAP else 1 - d[1]
            src = coltx.at[turn, side, source]
            dst = colrx.at[turn, side, level, goal]
        else:
            side = side_of("gy", d[1])
            src = rowtx.at[turn, side, source]
            dst = rowrx.at[turn, side, goal]
        return remote(turn, d, src, dst, toward)

    def face_copy(turn, d, first, count, toward=None):
        source, goal = planes(d[0])
        if d[0] == SWAP:
            inner = pl.ds(1 + (n0 - 1) * (1 - place["gx"]), 1)
        else:
            inner = pl.ds(n0 if d[0] > 0 else 1, 1)
        part = (turn, pl.ds(first, count))
        src = field.at[part + (inner, pl.ds(0, n1), pl.ds(0, n2))]
        dst = field.at[part + (goal, pl.ds(0, n1), pl.ds(0, n2))]
        return remote(turn, d, src, dst, toward)

    def face_start(turn, first, count):
        for d in faces:
            when(present(d), lambda: face_copy(turn, d, first, count).start())

    def pack(turn, count):
        for p in range(n0):
            low = jnp.zeros((n1, 128), jnp.float32)
            high = jnp.zeros((n1, 128), jnp.float32)
            for f in range(count):
                block = field[turn, f, 1 + p, 0:n1, 0:n2]
                rowtx[turn, 0, p, f : f + 1, :] = block[n1 - 1 : n1]
                rowtx[turn, 1, p, f : f + 1, :] = block[0:1]
                high = jnp.where(lane == f, block[:, n2 - 1 : n2], high)
                low = jnp.where(lane == f, block[:, 0:1], low)
            coltx[turn, 0, p] = high
            coltx[turn, 1, p] = low

    def halo_start(turn):
        for d in packed:
            when(present(d), lambda: pack_copy(turn, d).start())

    def halo_finish(turn, count):
        for d in packed:
            when(present(opposite(d)), lambda: pack_copy(turn, d, opposite(d)).wait_recv())
        for d in faces:
            when(present(opposite(d)), lambda: face_copy(turn, d, 0, count, opposite(d)).wait_recv())
        for d in packed:
            when(present(d), lambda: pack_copy(turn, d).wait_send())
        for d in faces:
            when(present(d), lambda: face_copy(turn, d, 0, count).wait_send())

        def unpack(q, carry):
            for f in range(count):
                low, high = rowrx[turn, 0, q, f : f + 1, :], rowrx[turn, 1, q, f : f + 1, :]
                field[turn, f, q, n1 : n1 + 8, 0:n2] = jnp.where(row == 0, high, jnp.where(row == 7, low, 0.0))
                for yy, top, size in ((1, 0, n1), (None, n1, 8)):
                    if yy is None:
                        first = colrx[turn, 1, 2, q, 0:1, f : f + 1]
                        last = colrx[turn, 1, 0, q, n1 - 1 : n1, f : f + 1]
                        after = jnp.where(row[:, 0:1] == 0, first, jnp.where(row[:, 0:1] == 7, last, 0.0))
                        first = colrx[turn, 0, 2, q, 0:1, f : f + 1]
                        last = colrx[turn, 0, 0, q, n1 - 1 : n1, f : f + 1]
                        before = jnp.where(row[:, 0:1] == 0, first, jnp.where(row[:, 0:1] == 7, last, 0.0))
                    else:
                        after = colrx[turn, 1, 1, q, :, f : f + 1]
                        before = colrx[turn, 0, 1, q, :, f : f + 1]
                    where = lane[0:1] if size != n1 else lane
                    field[turn, f, q, top : top + size, n2 : n2 + 128] = jnp.where(
                        where == 0, after, jnp.where(where == 127, before, 0.0)
                    )
            return carry

        lax.fori_loop(0, n0 + 2, unpack, 0)

    def sum_start(turn, step, tile):
        stage = stages[step]
        index, size = members(stage)
        sumtx[turn, step] = tile
        sumrx[turn, step, pl.ds(index, 1)] = tile[None]
        for offset in range(1, size):
            pltpu.make_async_remote_copy(
                src_ref=sumtx.at[turn, step],
                dst_ref=sumrx.at[turn, step, index],
                send_sem=sum_send.at[turn, step], recv_sem=sum_recv.at[turn, step],
                device_id=peer(stage, lax.rem(index + offset, size)), device_id_type=MESH,
            ).start()

    def sum_wait(turn, step):
        stage = stages[step]
        index, size = members(stage)
        if size > 1:
            whole = sumrx.at[turn, step, pl.ds(0, size - 1)]
            return pltpu.make_async_remote_copy(
                src_ref=whole, dst_ref=whole,
                send_sem=sum_send.at[turn, step], recv_sem=sum_recv.at[turn, step],
                device_id=peer(stage, lax.rem(index + 1, size)), device_id_type=MESH,
            )

    def sum_finish(turn):
        for step, stage in enumerate(stages):
            _, size = members(stage)
            if size > 1:
                sum_wait(turn, step).wait_recv()
            total = sumrx[turn, step, 0]
            for number in range(1, size):
                total = total + sumrx[turn, step, number]
            if step + 1 < len(stages):
                sum_start(turn, step + 1, total)
        spots = lax.broadcasted_iota(jnp.int32, (grams.shape[0], 128), 0)
        across = lax.broadcasted_iota(jnp.int32, (grams.shape[0], 128), 1)
        spread = jnp.where(spots == across, total[0:1], 0.0)
        grams[...] = jnp.broadcast_to(jnp.sum(spread, axis=1, keepdims=True), grams.shape)

    def gram_rows(first, other, pairs, base):
        for number, (i, j) in enumerate(pairs):
            product = None
            for d in range(3):
                for p in range(n0):
                    term = first[i, d, p] * other[j, d, p]
                    product = term if product is None else product + term
            grams[base + number : base + number + 1, :] = jnp.sum(product, axis=0, keepdims=True)

    def gram_tile():
        return lax.dot_general(
            jnp.ones((8, 128), jnp.float32), grams[...], (((1,), (1,)), ((), ())),
            precision=lax.Precision.HIGHEST, preferred_element_type=jnp.float32,
        )

    def apply(turn, finish, after=None):
        def one(c, carry):
            def plane(q):
                parts = {}
                for d in range(3):
                    v = field[turn, 3 * c + d, q]
                    after = pltpu.roll(v, lanes - 1, 1)
                    for cc, along in enumerate((v + after, after - v)):
                        beyond = pltpu.roll(along, rows - 1, 0)
                        parts[d, 0, cc] = along + beyond
                        parts[d, 1, cc] = beyond - along
                return parts

            before, behind = plane(0), None
            for q in range(n0 + 1):
                ahead = plane(q + 1)
                strain = {}
                for d, b, cc in ahead:
                    strain[4 * 0 + 2 * b + cc, d] = ahead[d, b, cc] + before[d, b, cc]
                    strain[4 * 1 + 2 * b + cc, d] = ahead[d, b, cc] - before[d, b, cc]
                stiff = modulus[q]
                stress = {}
                for number in range(8):
                    for d in range(3):
                        total = None
                        for other in range(8):
                            for e in range(3):
                                weight = modes[3 * number + d, 3 * other + e]
                                if weight != 0.0:
                                    term = float(weight) * strain[other, e]
                                    total = term if total is None else total + term
                        stress[number, d] = None if total is None else total * stiff

                def side(sign):
                    out = {}
                    for d in range(3):
                        for b in range(2):
                            for cc in range(2):
                                total, change = stress[2 * b + cc, d], stress[4 + 2 * b + cc, d]
                                if total is None:
                                    out[d, b, cc] = change if sign > 0 else -change
                                else:
                                    out[d, b, cc] = total + change if sign > 0 else total - change
                    return out

                if q > 0:
                    near = side(-1)
                    for d in range(3):
                        folded = []
                        for cc in range(2):
                            flat = behind[d, 0, cc] + near[d, 0, cc]
                            tilt = behind[d, 1, cc] + near[d, 1, cc]
                            folded.append((flat - tilt)[0:n1] + pltpu.roll(flat + tilt, 1, 0)[0:n1])
                        force = (folded[0] - folded[1])[:, 0:n2]
                        force = force + pltpu.roll(folded[0] + folded[1], 1, 1)[:, 0:n2]
                        finish(c, d, q - 1, force)
                if q < n0:
                    behind = side(1)
                before = ahead
            if after is not None:
                after(c)
            return carry

        lax.fori_loop(0, cases, one, 0)

    for copy in loaded[:3]:
        copy.wait()
    for p in range(n0):
        density = (design[p].astype(jnp.float32) + 1.0) * (1.0 / LEVELS)
        movable_ref[p] = 1.0 - supports[p].astype(jnp.float32)
        field[0, fields, 1 + p, 0:n1, 0:n2] = soft_modulus + (1.0 - soft_modulus) * density * density * density
    for c in range(cases):
        for d in range(3):
            for p in range(n0):
                field[0, 3 * c + d, 1 + p, 0:n1, 0:n2] = movable_ref[p] * start[c, d, p]
    pack(0, fields + 1)
    pl.semaphore_wait(barrier, expected)
    halo_start(0)
    face_start(0, 0, fields + 1)
    loaded[3].wait()

    along1, along2 = n1 * sizes["gy"], n2 * sizes["gz"]

    def load_case(c, carry):
        for p in range(n0):
            first = place["gx"] * n0 + p
            second_index = place["gy"] * n1 + lax.broadcasted_iota(jnp.int32, (n1, n2), 0)
            third = place["gz"] * n2 + lax.broadcasted_iota(jnp.int32, (n1, n2), 1)
            number = (first * along1 + second_index) * along2 + third
            sums = [body[c, d, p] for d in range(3)]
            for l in range(loads):
                hit = number == nodes[c, l]
                for d in range(3):
                    sums[d] = sums[d] + jnp.where(hit, values[c, l, d], 0.0)
            for d in range(3):
                resid[c, d, p] = movable_ref[p] * sums[d]
        return carry

    lax.fori_loop(0, cases, load_case, 0)
    halo_finish(0, fields + 1)
    for q in range(n0 + 1):
        modulus[q] = field[0, fields, q]
    for p in range(n0):
        total = modulus[p] + modulus[p + 1]
        total = total + pltpu.roll(total, 1, 0)
        total = total + pltpu.roll(total, 1, 1)
        movable = movable_ref[p]
        guarded = jnp.where(movable > 0, total[0:n1, 0:n2], 1.0)
        scale_ref[p] = movable / (corner_stiffness * guarded) + (1.0 - movable)

    def first_finish(c, d, p, force):
        movable = movable_ref[p]
        value = resid[c, d, p] - (movable * force + (1.0 - movable) * start[c, d, p])
        resid[c, d, p] = value
        direction = scale_ref[p] * value
        direct[c, d, p] = direction
        field[1, 3 * c + d, 1 + p, 0:n1, 0:n2] = movable * direction

    apply(0, first_finish, lambda c: face_start(1, 3 * c, 3))
    pack(1, fields)
    halo_start(1)
    pairs = triangle(cases)
    count = len(pairs)
    grams[...] = jnp.zeros_like(grams)
    gram_rows(direct, resid, pairs, count)
    halo_finish(1, fields)

    def second_finish(c, d, p, force):
        movable = movable_ref[p]
        value = movable * force + (1.0 - movable) * direct[c, d, p]
        image[c, d, p] = value
        scaled = scale_ref[p] * value
        second[c, d, p] = scaled
        field[2, 3 * c + d, 1 + p, 0:n1, 0:n2] = movable * scaled

    apply(1, second_finish, lambda c: face_start(2, 3 * c, 3))
    pack(2, fields)
    halo_start(2)
    gram_rows(direct, image, pairs, 0)
    gram_rows(image, second, pairs, 2 * count)
    sum_start(0, 0, gram_tile())
    halo_finish(2, fields)

    def third_finish(c, d, p, force):
        movable = movable_ref[p]
        second_image[c, d, p] = movable * force + (1.0 - movable) * second[c, d, p]

    apply(2, third_finish)
    sum_finish(0)

    def entries(base):
        spot = {}
        for number, (i, j) in enumerate(pairs):
            spot[i, j] = spot[j, i] = base + number
        return lambda i, j: grams[spot[i, j] : spot[i, j] + 1, :]

    everyone = [(i, j) for i in range(cases) for j in range(cases)]
    curvature, projection, crossing = entries(0), entries(count), entries(2 * count)
    factor = spd_factor(curvature, cases)
    step = spd_solve(factor, {pair: projection(*pair) for pair in everyone}, cases)
    coupling = {}
    for i, j in everyone:
        total = curvature(j, i)
        for k in range(cases):
            total = total - crossing(i, k) * step[k, j]
        coupling[i, j] = total
    beta = spd_solve(factor, coupling, cases)
    for number, pair in enumerate(everyone):
        coef[0, number] = jnp.broadcast_to(step[pair], coef.shape[2:])
        coef[1, number] = jnp.broadcast_to(beta[pair], coef.shape[2:])

    def first_update(number, carry):
        d, p = lax.div(number, n0), lax.rem(number, n0)
        scale = scale_ref[p]
        for i in range(cases):
            gain, loss, kept, moved = start[i, d, p], resid[i, d, p], None, image[i, d, p]
            for j in range(cases):
                alpha, weight = coef[0, j * cases + i], coef[1, j * cases + i]
                gain = gain + direct[j, d, p] * alpha
                loss = loss - image[j, d, p] * alpha
                term = direct[j, d, p] * weight
                kept = term if kept is None else kept + term
                moved = moved - (second_image[j, d, p] * alpha + image[j, d, p] * weight)
            solution_ref[i, d, p] = gain
            residual_ref[i, d, p] = loss
            field[0, 3 * i + d, 1 + p, 0:n1, 0:n2] = scale * loss - kept
            field[1, 3 * i + d, 1 + p, 0:n1, 0:n2] = moved
        for i in range(cases):
            second[i, d, p] = field[0, 3 * i + d, 1 + p, 0:n1, 0:n2]
            second_image[i, d, p] = field[1, 3 * i + d, 1 + p, 0:n1, 0:n2]
        return carry

    lax.fori_loop(0, 3 * n0, first_update, 0)
    grams[...] = jnp.zeros_like(grams)
    gram_rows(second, second_image, pairs, 0)
    gram_rows(second, residual_ref, everyone, count)
    sum_start(1, 0, gram_tile())
    sum_finish(1)
    curvature = entries(0)
    factor = spd_factor(curvature, cases)
    right = {pair: grams[count + n : count + n + 1, :] for n, pair in enumerate(everyone)}
    step = spd_solve(factor, right, cases)
    for number, pair in enumerate(everyone):
        coef[0, number] = jnp.broadcast_to(step[pair], coef.shape[2:])

    def second_update(number, carry):
        d, p = lax.div(number, n0), lax.rem(number, n0)
        for i in range(cases):
            gain, loss = solution_ref[i, d, p], residual_ref[i, d, p]
            for j in range(cases):
                alpha = coef[0, j * cases + i]
                gain = gain + second[j, d, p] * alpha
                loss = loss - second_image[j, d, p] * alpha
            solution_ref[i, d, p] = gain
            residual_ref[i, d, p] = loss
        return carry

    lax.fori_loop(0, 3 * n0, second_update, 0)
    for turn in range(2):
        for number, stage in enumerate(stages):
            _, size = members(stage)
            if size > 1:
                sum_wait(turn, number).wait_send()


def solution(mesh):
    sizes = {axis: mesh.shape[axis] for axis in AXES}
    group = sizes["gx"] * sizes["gy"] * sizes["gz"]
    stages = [AXES] if group <= 16 else [("gz",), ("gy",), ("gx",)]

    def shards(design, supports, body_load, start, load_nodes, load_values):
        cases, _, n0, n1, n2 = start.shape
        fields = 3 * cases
        padded = -(-(fields + 1) // 8) * 8
        directions = max(len(neighbours(sizes)), 1)
        widest = max(int(np.prod([sizes[axis] for axis in stage])) for stage in stages)
        f32 = jnp.float32
        vmem, smem = pl.BlockSpec(memory_space=pltpu.VMEM), pl.BlockSpec(memory_space=pltpu.SMEM)
        block = pltpu.VMEM(start.shape, f32)
        gram_count = -(-max(3 * cases * (cases + 1) // 2, cases * (cases + 1) // 2 + cases * cases) // 128) * 128
        scratch = [
            pltpu.VMEM((n0, n1, n2), jnp.int32),
            pltpu.VMEM((n0, n1, n2), jnp.int32),
            block,
            block,
            pltpu.VMEM((3, fields + 1, n0 + 2, n1 + 8, n2 + 128), f32),
            pltpu.VMEM((3, 2, n0, padded, n2), f32),
            pltpu.VMEM((3, 2, n0 + 2, padded, n2), f32),
            pltpu.VMEM((3, 2, n0, n1, 128), f32),
            pltpu.VMEM((3, 2, 3, n0 + 2, n1, 128), f32),
            pltpu.VMEM((n0, n1, n2), f32),
            pltpu.VMEM((n0, n1, n2), f32),
            pltpu.VMEM((n0 + 1, n1 + 8, n2 + 128), f32),
            block, block, block, block, block,
            pltpu.VMEM((gram_count, 128), f32),
            pltpu.VMEM((2, cases * cases, n1, n2), f32),
            pltpu.VMEM((2, len(stages), 8, 128), f32),
            pltpu.VMEM((2, len(stages), widest, 8, 128), f32),
            pltpu.SemaphoreType.DMA((directions,)),
            pltpu.SemaphoreType.DMA((3, directions)),
            pltpu.SemaphoreType.DMA((2, len(stages))),
            pltpu.SemaphoreType.DMA((2, len(stages))),
            pltpu.SemaphoreType.DMA((4,)),
        ]
        return pl.pallas_call(
            functools.partial(kernel, sizes, stages),
            out_shape=(jax.ShapeDtypeStruct(start.shape, f32), jax.ShapeDtypeStruct(start.shape, f32)),
            in_specs=[pl.BlockSpec(memory_space=pltpu.HBM)] * 4 + [smem] * 2,
            out_specs=(vmem, vmem),
            scratch_shapes=scratch,
            compiler_params=pltpu.CompilerParams(collective_id=0, has_side_effects=True),
        )(design, supports, body_load, start, load_nodes, load_values)

    in_specs = (
        P(("grp", "gx"), "gy", "gz"),
        P(("grp", "gx"), "gy", "gz"),
        P("grp", None, "gx", "gy", "gz"),
        P("grp", None, "gx", "gy", "gz"),
        P("grp", None),
        P("grp", None, None),
    )
    out_specs = (P("grp", None, "gx", "gy", "gz"), P("grp", None, "gx", "gy", "gz"))
    return jax.shard_map(shards, mesh=mesh, in_specs=in_specs, out_specs=out_specs, check_vma=False)
```

```python
import functools
import itertools

import jax
import jax.numpy as jnp
import numpy as np
from jax import lax
from jax.experimental import pallas as pl
from jax.experimental.pallas import tpu as pltpu
from jax.sharding import PartitionSpec as P

LEVELS = 16
AXES = ("gx", "gy", "gz")
MESH = pl.DeviceIdType.MESH
soft_modulus = 0.05
poisson_ratio = 0.3
SWAP = 2


def neighbours(sizes):
    options = [(0,) if sizes[axis] == 1 else (0, SWAP) if sizes[axis] == 2 else (-1, 0, 1) for axis in AXES]
    return [d for d in itertools.product(*options) if any(d)]


def corner_list():
    return [(first, second, third) for first in (0, 1) for second in (0, 1) for third in (0, 1)]


def element_matrix():
    lame_first = poisson_ratio / ((1.0 + poisson_ratio) * (1.0 - 2.0 * poisson_ratio))
    shear_modulus = 1.0 / (2.0 * (1.0 + poisson_ratio))
    elastic = np.zeros((6, 6))
    elastic[:3, :3] = lame_first
    for axis_dim in range(3):
        elastic[axis_dim, axis_dim] += 2.0 * shear_modulus
        elastic[3 + axis_dim, 3 + axis_dim] = shear_modulus
    gauss_points = [0.5 - 0.5 / np.sqrt(3.0), 0.5 + 0.5 / np.sqrt(3.0)]
    corners = corner_list()
    matrix_total = np.zeros((24, 24))
    for first_point in gauss_points:
        for second_point in gauss_points:
            for third_point in gauss_points:
                points = (first_point, second_point, third_point)
                strain = np.zeros((6, 24))
                for number, corner in enumerate(corners):
                    values = [
                        points[axis_dim] if corner[axis_dim] else 1.0 - points[axis_dim]
                        for axis_dim in range(3)
                    ]
                    slopes = [1.0 if corner[axis_dim] else -1.0 for axis_dim in range(3)]
                    grad_first = slopes[0] * values[1] * values[2]
                    grad_second = values[0] * slopes[1] * values[2]
                    grad_third = values[0] * values[1] * slopes[2]
                    column = 3 * number
                    strain[0, column] = grad_first
                    strain[1, column + 1] = grad_second
                    strain[2, column + 2] = grad_third
                    strain[3, column] = grad_second
                    strain[3, column + 1] = grad_first
                    strain[4, column + 1] = grad_third
                    strain[4, column + 2] = grad_second
                    strain[5, column] = grad_third
                    strain[5, column + 2] = grad_first
                matrix_total = matrix_total + strain.T @ elastic @ strain / 8.0
    return matrix_total


def mode_matrix():
    matrix = element_matrix()
    pair = np.array([[1.0, 1.0], [-1.0, 1.0]])
    basis = np.kron(np.kron(np.kron(pair, pair), pair), np.eye(3))
    inverse = np.linalg.inv(basis)
    modes = inverse.T @ matrix @ inverse
    modes[np.abs(modes) < 1e-9] = 0.0
    return float(np.float32(matrix[0, 0])), modes


def triangle(count):
    return [(i, j) for i in range(count) for j in range(i, count)]


def spd_factor(entry, count):
    lower, inverse = {}, []
    work = {(i, j): entry(j, i) for i in range(count) for j in range(i + 1)}
    for k in range(count):
        inverse.append(1.0 / work[k, k])
        for i in range(k + 1, count):
            lower[i, k] = work[i, k] * inverse[k]
        for i in range(k + 1, count):
            for j in range(k + 1, i + 1):
                work[i, j] = work[i, j] - lower[i, k] * work[j, k]
    return lower, inverse


def spd_solve(factor, right, count):
    lower, inverse = factor
    result = {}
    for column in range(count):
        values = [right[row, column] for row in range(count)]
        for i in range(count):
            for k in range(i):
                values[i] = values[i] - lower[i, k] * values[k]
        values = [value * scale for value, scale in zip(values, inverse)]
        for i in reversed(range(count)):
            for k in range(i + 1, count):
                values[i] = values[i] - lower[k, i] * values[k]
        for row in range(count):
            result[row, column] = values[row]
    return result


def kernel(
    sizes, stages,
    design_hbm, supports_hbm, body_hbm, start_hbm, nodes, values,
    solution_ref, residual_ref, design, supports, body, start,
    field, rowtx, rowrx, coltx, colrx, movable_ref, scale_ref, modulus,
    resid, direct, image, second, second_image, grams, coef, sumtx, sumrx,
    halo_send, halo_recv, sum_send, sum_recv, load_sem,
):
    cases, _, n0, n1, n2 = start.shape
    loads = nodes.shape[1]
    fields = 3 * cases
    rows, lanes = field.shape[-2:]
    corner_stiffness, modes = mode_matrix()
    place = {axis: lax.axis_index(axis) for axis in AXES}

    def present(d):
        inside = None
        for axis, step in zip(AXES, d):
            if step in (-1, 1):
                test = (place[axis] > 0) if step < 0 else (place[axis] < sizes[axis] - 1)
                inside = test if inside is None else jnp.logical_and(inside, test)
        return inside

    def when(condition, run):
        if condition is None:
            run()
        else:
            pl.when(condition)(run)

    def target(d):
        return {
            axis: 1 - place[axis] if step == SWAP else place[axis] + step
            for axis, step in zip(AXES, d) if step
        }

    def opposite(d):
        return tuple(step if step == SWAP else -step for step in d)

    directions = neighbours(sizes)
    faces = [d for d in directions if d[0] and not d[1] and not d[2]]
    packed = [d for d in directions if d not in faces]

    def members(stage):
        index, size = 0, 1
        for axis in stage:
            index = index * sizes[axis] + place[axis]
            size = size * sizes[axis]
        return index, size

    def peer(stage, number):
        out = {}
        for axis in reversed(stage):
            out[axis] = lax.rem(number, sizes[axis])
            number = lax.div(number, sizes[axis])
        return out

    loaded = [
        pltpu.make_async_copy(source, goal, load_sem.at[number])
        for number, (source, goal) in enumerate(
            ((start_hbm, start), (supports_hbm, supports), (design_hbm, design), (body_hbm, body))
        )
    ]
    for copy in loaded:
        copy.start()
    barrier = pltpu.get_barrier_semaphore()
    if any(sizes[axis] > 1 for axis in AXES):
        rowrx[...] = jnp.zeros_like(rowrx)
        colrx[...] = jnp.zeros_like(colrx)
        for turn in range(3):
            zero = jnp.zeros((field.shape[1], 1, n1, n2), jnp.float32)
            field[turn, :, 0:1, 0:n1, 0:n2] = zero
            field[turn, :, n0 + 1 : n0 + 2, 0:n1, 0:n2] = zero
    expected = 0
    for stage in stages:
        index, size = members(stage)
        expected = expected + (size - 1)
        for offset in range(1, size):
            pl.semaphore_signal(
                barrier, inc=1, device_id=peer(stage, lax.rem(index + offset, size)), device_id_type=MESH
            )
    if len(stages) > 1:
        for d in directions:
            exists = present(d)
            expected = expected + (1 if exists is None else exists.astype(jnp.int32))

            def greet():
                pl.semaphore_signal(barrier, inc=1, device_id=target(d), device_id_type=MESH)

            when(exists, greet)

    lane = lax.broadcasted_iota(jnp.int32, (n1, 128), 1)
    row = lax.broadcasted_iota(jnp.int32, (8, n2), 0)

    def planes(step):
        if step == 0:
            return pl.ds(0, n0), pl.ds(1, n0)
        if step == SWAP:
            return pl.ds((n0 - 1) * (1 - place["gx"]), 1), pl.ds((n0 + 1) * place["gx"], 1)
        if step > 0:
            return pl.ds(n0 - 1, 1), pl.ds(0, 1)
        return pl.ds(0, 1), pl.ds(n0 + 1, 1)

    def side_of(axis, step):
        return place[axis] if step == SWAP else (0 if step > 0 else 1)

    def remote(turn, d, src, dst, toward):
        number = directions.index(d)
        return pltpu.make_async_remote_copy(
            src_ref=src, dst_ref=dst,
            send_sem=halo_send.at[number], recv_sem=halo_recv.at[turn, number],
            device_id=target(toward or d), device_id_type=MESH,
        )

    def pack_copy(turn, d, toward=None):
        source, goal = planes(d[0])
        if d[2]:
            side = side_of("gz", d[2])
            level = 2 * place["gy"] if d[1] == SWAP else 1 - d[1]
            src = coltx.at[turn, side, source]
            dst = colrx.at[turn, side, level, goal]
        else:
            side = side_of("gy", d[1])
            src = rowtx.at[turn, side, source]
            dst = rowrx.at[turn, side, goal]
        return remote(turn, d, src, dst, toward)

    def face_copy(turn, d, first, count, toward=None):
        source, goal = planes(d[0])
        if d[0] == SWAP:
            inner = pl.ds(1 + (n0 - 1) * (1 - place["gx"]), 1)
        else:
            inner = pl.ds(n0 if d[0] > 0 else 1, 1)
        part = (turn, pl.ds(first, count))
        src = field.at[part + (inner, pl.ds(0, n1), pl.ds(0, n2))]
        dst = field.at[part + (goal, pl.ds(0, n1), pl.ds(0, n2))]
        return remote(turn, d, src, dst, toward)

    def face_start(turn, first, count):
        for d in faces:
            when(present(d), lambda: face_copy(turn, d, first, count).start())

    def pack(turn, count):
        for p in range(n0):
            low = jnp.zeros((n1, 128), jnp.float32)
            high = jnp.zeros((n1, 128), jnp.float32)
            for f in range(count):
                block = field[turn, f, 1 + p, 0:n1, 0:n2]
                rowtx[turn, 0, p, f : f + 1, :] = block[n1 - 1 : n1]
                rowtx[turn, 1, p, f : f + 1, :] = block[0:1]
                high = jnp.where(lane == f, block[:, n2 - 1 : n2], high)
                low = jnp.where(lane == f, block[:, 0:1], low)
            coltx[turn, 0, p] = high
            coltx[turn, 1, p] = low

    def halo_start(turn):
        for d in packed:
            when(present(d), lambda: pack_copy(turn, d).start())

    def halo_finish(turn, count):
        for d in packed:
            when(present(opposite(d)), lambda: pack_copy(turn, d, opposite(d)).wait_recv())
        def unpack(q, carry):
            edge = lax.broadcasted_iota(jnp.int32, (8, 128), 0)
            across = lax.broadcasted_iota(jnp.int32, (8, 128), 1)
            corners = [
                jnp.where(
                    edge == 0, colrx[turn, side, 2, q, 0:1, :],
                    jnp.where(edge == 7, colrx[turn, side, 0, q, n1 - 1 : n1, :], 0.0),
                )
                for side in range(2)
            ]
            sides = [colrx[turn, side, 1, q] for side in range(2)]
            for f in range(count):
                low, high = rowrx[turn, 0, q, f : f + 1, :], rowrx[turn, 1, q, f : f + 1, :]
                field[turn, f, q, n1 : n1 + 8, 0:n2] = jnp.where(row == 0, high, jnp.where(row == 7, low, 0.0))
                for (before, after), where, top, size in ((sides, lane, 0, n1), (corners, across, n1, 8)):
                    field[turn, f, q, top : top + size, n2 : n2 + 128] = jnp.where(
                        where == 0, after[:, f : f + 1], jnp.where(where == 127, before[:, f : f + 1], 0.0)
                    )
            return carry

        lax.fori_loop(0, n0 + 2, unpack, 0)
        for d in faces:
            when(present(opposite(d)), lambda: face_copy(turn, d, 0, count, opposite(d)).wait_recv())
        for d in packed:
            when(present(d), lambda: pack_copy(turn, d).wait_send())
        for d in faces:
            when(present(d), lambda: face_copy(turn, d, 0, count).wait_send())

    def sum_start(turn, step, tile):
        stage = stages[step]
        index, size = members(stage)
        sumtx[turn, step] = tile
        sumrx[turn, step, pl.ds(index, 1)] = tile[None]
        for offset in range(1, size):
            pltpu.make_async_remote_copy(
                src_ref=sumtx.at[turn, step],
                dst_ref=sumrx.at[turn, step, index],
                send_sem=sum_send.at[turn, step], recv_sem=sum_recv.at[turn, step],
                device_id=peer(stage, lax.rem(index + offset, size)), device_id_type=MESH,
            ).start()

    def sum_wait(turn, step):
        stage = stages[step]
        index, size = members(stage)
        if size > 1:
            whole = sumrx.at[turn, step, pl.ds(0, size - 1)]
            return pltpu.make_async_remote_copy(
                src_ref=whole, dst_ref=whole,
                send_sem=sum_send.at[turn, step], recv_sem=sum_recv.at[turn, step],
                device_id=peer(stage, lax.rem(index + 1, size)), device_id_type=MESH,
            )

    def sum_finish(turn):
        for step, stage in enumerate(stages):
            _, size = members(stage)
            if size > 1:
                sum_wait(turn, step).wait_recv()
            total = sumrx[turn, step, 0]
            for number in range(1, size):
                total = total + sumrx[turn, step, number]
            if step + 1 < len(stages):
                sum_start(turn, step + 1, total)
        spots = lax.broadcasted_iota(jnp.int32, (grams.shape[0], 128), 0)
        across = lax.broadcasted_iota(jnp.int32, (grams.shape[0], 128), 1)
        spread = jnp.where(spots == across, total[0:1], 0.0)
        grams[...] = jnp.broadcast_to(jnp.sum(spread, axis=1, keepdims=True), grams.shape)

    def gram_rows(first, other, pairs, base):
        for number, (i, j) in enumerate(pairs):
            product = None
            for d in range(3):
                for p in range(n0):
                    term = first[i, d, p] * other[j, d, p]
                    product = term if product is None else product + term
            grams[base + number : base + number + 1, :] = jnp.sum(product, axis=0, keepdims=True)

    def gram_tile():
        return lax.dot_general(
            jnp.ones((8, 128), jnp.float32), grams[...], (((1,), (1,)), ((), ())),
            precision=lax.Precision.HIGHEST, preferred_element_type=jnp.float32,
        )

    def apply(turn, finish, after=None):
        def one(c, carry):
            def plane(q):
                parts = {}
                for d in range(3):
                    v = field[turn, 3 * c + d, q]
                    after = pltpu.roll(v, lanes - 1, 1)
                    for cc, along in enumerate((v + after, after - v)):
                        beyond = pltpu.roll(along, rows - 1, 0)
                        parts[d, 0, cc] = along + beyond
                        parts[d, 1, cc] = beyond - along
                return parts

            before, behind = plane(0), None
            for q in range(n0 + 1):
                ahead = plane(q + 1)
                strain = {}
                for d, b, cc in ahead:
                    strain[4 * 0 + 2 * b + cc, d] = ahead[d, b, cc] + before[d, b, cc]
                    strain[4 * 1 + 2 * b + cc, d] = ahead[d, b, cc] - before[d, b, cc]
                stiff = modulus[q]
                stress = {}
                for number in range(8):
                    for d in range(3):
                        total = None
                        for other in range(8):
                            for e in range(3):
                                weight = modes[3 * number + d, 3 * other + e]
                                if weight != 0.0:
                                    term = float(weight) * strain[other, e]
                                    total = term if total is None else total + term
                        stress[number, d] = None if total is None else total * stiff

                def side(sign):
                    out = {}
                    for d in range(3):
                        for b in range(2):
                            for cc in range(2):
                                total, change = stress[2 * b + cc, d], stress[4 + 2 * b + cc, d]
                                if total is None:
                                    out[d, b, cc] = change if sign > 0 else -change
                                else:
                                    out[d, b, cc] = total + change if sign > 0 else total - change
                    return out

                if q > 0:
                    near = side(-1)
                    for d in range(3):
                        folded = []
                        for cc in range(2):
                            flat = behind[d, 0, cc] + near[d, 0, cc]
                            tilt = behind[d, 1, cc] + near[d, 1, cc]
                            folded.append((flat - tilt)[0:n1] + pltpu.roll(flat + tilt, 1, 0)[0:n1])
                        force = (folded[0] - folded[1])[:, 0:n2]
                        force = force + pltpu.roll(folded[0] + folded[1], 1, 1)[:, 0:n2]
                        finish(c, d, q - 1, force)
                if q < n0:
                    behind = side(1)
                before = ahead
            if after is not None:
                after(c)
            return carry

        lax.fori_loop(0, cases, one, 0)

    for copy in loaded[:3]:
        copy.wait()
    for p in range(n0):
        density = (design[p].astype(jnp.float32) + 1.0) * (1.0 / LEVELS)
        movable_ref[p] = 1.0 - supports[p].astype(jnp.float32)
        field[0, fields, 1 + p, 0:n1, 0:n2] = soft_modulus + (1.0 - soft_modulus) * density * density * density
    for c in range(cases):
        for d in range(3):
            for p in range(n0):
                field[0, 3 * c + d, 1 + p, 0:n1, 0:n2] = movable_ref[p] * start[c, d, p]
    pack(0, fields + 1)
    pl.semaphore_wait(barrier, expected)
    halo_start(0)
    face_start(0, 0, fields + 1)
    loaded[3].wait()

    along1, along2 = n1 * sizes["gy"], n2 * sizes["gz"]

    def load_case(c, carry):
        for p in range(n0):
            first = place["gx"] * n0 + p
            second_index = place["gy"] * n1 + lax.broadcasted_iota(jnp.int32, (n1, n2), 0)
            third = place["gz"] * n2 + lax.broadcasted_iota(jnp.int32, (n1, n2), 1)
            number = (first * along1 + second_index) * along2 + third
            sums = [body[c, d, p] for d in range(3)]
            for l in range(loads):
                hit = number == nodes[c, l]
                for d in range(3):
                    sums[d] = sums[d] + jnp.where(hit, values[c, d, l], 0.0)
            for d in range(3):
                resid[c, d, p] = movable_ref[p] * sums[d]
        return carry

    lax.fori_loop(0, cases, load_case, 0)
    halo_finish(0, fields + 1)
    for q in range(n0 + 1):
        modulus[q] = field[0, fields, q]
    for p in range(n0):
        total = modulus[p] + modulus[p + 1]
        total = total + pltpu.roll(total, 1, 0)
        total = total + pltpu.roll(total, 1, 1)
        movable = movable_ref[p]
        guarded = jnp.where(movable > 0, total[0:n1, 0:n2], 1.0)
        scale_ref[p] = movable / (corner_stiffness * guarded) + (1.0 - movable)

    def first_finish(c, d, p, force):
        movable = movable_ref[p]
        value = resid[c, d, p] - (movable * force + (1.0 - movable) * start[c, d, p])
        resid[c, d, p] = value
        direction = scale_ref[p] * value
        direct[c, d, p] = direction
        field[1, 3 * c + d, 1 + p, 0:n1, 0:n2] = movable * direction

    apply(0, first_finish, lambda c: face_start(1, 3 * c, 3))
    pack(1, fields)
    halo_start(1)
    pairs = triangle(cases)
    count = len(pairs)
    grams[...] = jnp.zeros_like(grams)
    gram_rows(direct, resid, pairs, count)
    halo_finish(1, fields)

    def second_finish(c, d, p, force):
        movable = movable_ref[p]
        value = movable * force + (1.0 - movable) * direct[c, d, p]
        image[c, d, p] = value
        scaled = scale_ref[p] * value
        second[c, d, p] = scaled
        field[2, 3 * c + d, 1 + p, 0:n1, 0:n2] = movable * scaled

    apply(1, second_finish, lambda c: face_start(2, 3 * c, 3))
    pack(2, fields)
    halo_start(2)
    gram_rows(direct, image, pairs, 0)
    gram_rows(image, second, pairs, 2 * count)
    sum_start(0, 0, gram_tile())
    halo_finish(2, fields)

    def third_finish(c, d, p, force):
        movable = movable_ref[p]
        second_image[c, d, p] = movable * force + (1.0 - movable) * second[c, d, p]

    apply(2, third_finish)
    sum_finish(0)

    def entries(base):
        spot = {}
        for number, (i, j) in enumerate(pairs):
            spot[i, j] = spot[j, i] = base + number
        return lambda i, j: grams[spot[i, j] : spot[i, j] + 1, :]

    everyone = [(i, j) for i in range(cases) for j in range(cases)]
    curvature, projection, crossing = entries(0), entries(count), entries(2 * count)
    factor = spd_factor(curvature, cases)
    step = spd_solve(factor, {pair: projection(*pair) for pair in everyone}, cases)
    coupling = {}
    for i, j in everyone:
        total = curvature(j, i)
        for k in range(cases):
            total = total - crossing(i, k) * step[k, j]
        coupling[i, j] = total
    beta = spd_solve(factor, coupling, cases)
    for number, pair in enumerate(everyone):
        coef[0, number] = jnp.broadcast_to(step[pair], coef.shape[2:])
        coef[1, number] = jnp.broadcast_to(beta[pair], coef.shape[2:])

    def first_update(number, carry):
        d, p = lax.div(number, n0), lax.rem(number, n0)
        scale = scale_ref[p]
        for i in range(cases):
            gain, loss, kept, moved = start[i, d, p], resid[i, d, p], None, image[i, d, p]
            for j in range(cases):
                alpha, weight = coef[0, j * cases + i], coef[1, j * cases + i]
                gain = gain + direct[j, d, p] * alpha
                loss = loss - image[j, d, p] * alpha
                term = direct[j, d, p] * weight
                kept = term if kept is None else kept + term
                moved = moved - (second_image[j, d, p] * alpha + image[j, d, p] * weight)
            solution_ref[i, d, p] = gain
            residual_ref[i, d, p] = loss
            field[0, 3 * i + d, 1 + p, 0:n1, 0:n2] = scale * loss - kept
            field[1, 3 * i + d, 1 + p, 0:n1, 0:n2] = moved
        for i in range(cases):
            second[i, d, p] = field[0, 3 * i + d, 1 + p, 0:n1, 0:n2]
            second_image[i, d, p] = field[1, 3 * i + d, 1 + p, 0:n1, 0:n2]
        return carry

    lax.fori_loop(0, 3 * n0, first_update, 0)
    grams[...] = jnp.zeros_like(grams)
    gram_rows(second, second_image, pairs, 0)
    gram_rows(second, residual_ref, everyone, count)
    sum_start(1, 0, gram_tile())
    sum_finish(1)
    curvature = entries(0)
    factor = spd_factor(curvature, cases)
    right = {pair: grams[count + n : count + n + 1, :] for n, pair in enumerate(everyone)}
    step = spd_solve(factor, right, cases)
    for number, pair in enumerate(everyone):
        coef[0, number] = jnp.broadcast_to(step[pair], coef.shape[2:])

    def second_update(number, carry):
        d, p = lax.div(number, n0), lax.rem(number, n0)
        for i in range(cases):
            gain, loss = solution_ref[i, d, p], residual_ref[i, d, p]
            for j in range(cases):
                alpha = coef[0, j * cases + i]
                gain = gain + second[j, d, p] * alpha
                loss = loss - second_image[j, d, p] * alpha
            solution_ref[i, d, p] = gain
            residual_ref[i, d, p] = loss
        return carry

    lax.fori_loop(0, 3 * n0, second_update, 0)
    for turn in range(2):
        for number, stage in enumerate(stages):
            _, size = members(stage)
            if size > 1:
                sum_wait(turn, number).wait_send()


def solution(mesh):
    sizes = {axis: mesh.shape[axis] for axis in AXES}
    group = sizes["gx"] * sizes["gy"] * sizes["gz"]
    stages = [AXES] if group <= 16 else [("gz",), ("gy",), ("gx",)]

    def shards(design, supports, body_load, start, load_nodes, load_values):
        cases, _, n0, n1, n2 = start.shape
        fields = 3 * cases
        padded = -(-(fields + 1) // 8) * 8
        directions = max(len(neighbours(sizes)), 1)
        widest = max(int(np.prod([sizes[axis] for axis in stage])) for stage in stages)
        f32 = jnp.float32
        vmem, smem = pl.BlockSpec(memory_space=pltpu.VMEM), pl.BlockSpec(memory_space=pltpu.SMEM)
        block = pltpu.VMEM(start.shape, f32)
        gram_count = -(-max(3 * cases * (cases + 1) // 2, cases * (cases + 1) // 2 + cases * cases) // 128) * 128
        scratch = [
            pltpu.VMEM((n0, n1, n2), jnp.int32),
            pltpu.VMEM((n0, n1, n2), jnp.int32),
            block,
            block,
            pltpu.VMEM((3, fields + 1, n0 + 2, n1 + 8, n2 + 128), f32),
            pltpu.VMEM((3, 2, n0, padded, n2), f32),
            pltpu.VMEM((3, 2, n0 + 2, padded, n2), f32),
            pltpu.VMEM((3, 2, n0, n1, 128), f32),
            pltpu.VMEM((3, 2, 3, n0 + 2, n1, 128), f32),
            pltpu.VMEM((n0, n1, n2), f32),
            pltpu.VMEM((n0, n1, n2), f32),
            pltpu.VMEM((n0 + 1, n1 + 8, n2 + 128), f32),
            block, block, block, block, block,
            pltpu.VMEM((gram_count, 128), f32),
            pltpu.VMEM((2, cases * cases, n1, n2), f32),
            pltpu.VMEM((2, len(stages), 8, 128), f32),
            pltpu.VMEM((2, len(stages), widest, 8, 128), f32),
            pltpu.SemaphoreType.DMA((directions,)),
            pltpu.SemaphoreType.DMA((3, directions)),
            pltpu.SemaphoreType.DMA((2, len(stages))),
            pltpu.SemaphoreType.DMA((2, len(stages))),
            pltpu.SemaphoreType.DMA((4,)),
        ]
        return pl.pallas_call(
            functools.partial(kernel, sizes, stages),
            out_shape=(jax.ShapeDtypeStruct(start.shape, f32), jax.ShapeDtypeStruct(start.shape, f32)),
            in_specs=[pl.BlockSpec(memory_space=pltpu.HBM)] * 4 + [smem] * 2,
            out_specs=(vmem, vmem),
            scratch_shapes=scratch,
            compiler_params=pltpu.CompilerParams(collective_id=0, has_side_effects=True),
        )(design, supports, body_load, start, load_nodes, load_values.transpose(0, 2, 1))

    in_specs = (
        P(("grp", "gx"), "gy", "gz"),
        P(("grp", "gx"), "gy", "gz"),
        P("grp", None, "gx", "gy", "gz"),
        P("grp", None, "gx", "gy", "gz"),
        P("grp", None),
        P("grp", None, None),
    )
    out_specs = (P("grp", None, "gx", "gy", "gz"), P("grp", None, "gx", "gy", "gz"))
    return jax.shard_map(shards, mesh=mesh, in_specs=in_specs, out_specs=out_specs, check_vma=False)
```
